8 devices in a mesh: replica: 2 (over z, y), data: 4 (over x, core).
Axes of the slice: x: 2, y: 2, z: 1, core: 2. Of those that a mesh axis runs over, the one named last changes fastest.
Arguments:
- grad_w1: float32 [2, 3, 128, 512], P('replica', None, 'data')
- grad_w2: float32 [2, 3, 512, 128], P('replica', None, 'data')
- master_w1: float32 [3, 128, 512], P(None, 'data')
- master_w2: float32 [3, 512, 128], P(None, 'data')
- moment1_w1: float32 [3, 128, 512], P(None, 'data')
- moment1_w2: float32 [3, 512, 128], P(None, 'data')
- moment2_w1: float32 [3, 128, 512], P(None, 'data')
- moment2_w2: float32 [3, 512, 128], P(None, 'data')
- tokens: bfloat16 [65536, 128], P(('replica', 'data'))
- targets: bfloat16 [65536, 128], P(('replica', 'data'))
Outputs:
- output 1: float32 [65536], P(('replica', 'data'))
- output 2: bfloat16 [3, 128, 512], replicated
- output 3: bfloat16 [3, 512, 128], replicated
- output 4: float32 [3, 128, 512], P(None, 'data')
- output 5: float32 [3, 512, 128], P(None, 'data')
- output 6: float32 [3, 128, 512], P(None, 'data')
- output 7: float32 [3, 512, 128], P(None, 'data')
- output 8: float32 [3, 128, 512], P(None, 'data')
- output 9: float32 [3, 512, 128], P(None, 'data')
All inputs are finite; a program needn't handle non-finite values.
Results may differ from the reference program's by a relative error of at most 0.00480666.
Values are sent between devices in bfloat16 or wider.
A program may use at most 1 GiB of HBM per device.

```python
import jax
import jax.numpy as jnp
from jax import lax

D = 128
FF = 512
LAYERS = 3
BATCH = 65536
TOK_DEV = 8192
REPLICA = 2
STEP = 2

ADAM_BETA1 = 0.9
ADAM_BETA2 = 0.95
ADAM_EPS = 1e-8
WEIGHT_DECAY = 0.1
NORM_EPS = 1e-6
LEARN_RATE = 0.2 * D ** -0.5
GRAD_SCALE = 1e-3


def rms_norm(hidden):
    hidden_f32 = hidden.astype(jnp.float32)
    inv_rms = lax.rsqrt(jnp.mean(hidden_f32 * hidden_f32, axis=-1, keepdims=True) + NORM_EPS)
    return (hidden_f32 * inv_rms).astype(jnp.bfloat16)


def block_forward(hidden, w_up, w_down):
    normed = rms_norm(hidden)
    up_act = jnp.dot(normed, w_up, preferred_element_type=jnp.float32).astype(jnp.bfloat16)
    gelu_act = jax.nn.gelu(up_act.astype(jnp.float32), approximate=True).astype(jnp.bfloat16)
    down_out = jnp.dot(gelu_act, w_down, preferred_element_type=jnp.float32)
    return (hidden.astype(jnp.float32) + down_out).astype(jnp.bfloat16)


def stack_forward(tok_block, full_w1, full_w2):
    def layer_body(hidden, layer_w):
        return block_forward(hidden, layer_w[0], layer_w[1]), None
    return lax.scan(layer_body, tok_block, (full_w1, full_w2))[0]


def batch_forward(tokens, full_w1, full_w2):
    tok_blocks = tokens.reshape(BATCH // TOK_DEV, TOK_DEV, D)
    out_blocks = lax.map(lambda tok_block: stack_forward(tok_block, full_w1, full_w2), tok_blocks)
    return out_blocks.reshape(BATCH, D)


def batch_loss(tokens, targets, full_w1, full_w2):
    tok_blocks = tokens.reshape(BATCH // TOK_DEV, TOK_DEV, D)
    tgt_blocks = targets.reshape(BATCH // TOK_DEV, TOK_DEV, D)

    def block_loss(tok_pair):
        final_h = stack_forward(tok_pair[0], full_w1, full_w2).astype(jnp.float32)
        row_diff = final_h - tok_pair[1].astype(jnp.float32)
        return jnp.mean(row_diff * row_diff, axis=-1)

    return lax.map(block_loss, (tok_blocks, tgt_blocks)).reshape(BATCH)


def adam_update(grad_all, master, moment1, moment2):
    grad_mean = jnp.sum(grad_all, axis=0) / REPLICA
    new_m = ADAM_BETA1 * moment1 + (1.0 - ADAM_BETA1) * grad_mean
    new_v = ADAM_BETA2 * moment2 + (1.0 - ADAM_BETA2) * grad_mean * grad_mean
    corr_m = 1.0 - ADAM_BETA1 ** STEP
    corr_v = 1.0 - ADAM_BETA2 ** STEP
    step_dir = (new_m / corr_m) / (jnp.sqrt(new_v / corr_v) + ADAM_EPS)
    new_w = master - LEARN_RATE * (step_dir + WEIGHT_DECAY * master)
    return new_w, new_m, new_v


def setup_inputs(seed: int = 0) -> dict:
    rng_keys = jax.random.split(jax.random.key(seed), 10)
    shape_up = (LAYERS, D, FF)
    shape_down = (LAYERS, FF, D)
    grad_std = GRAD_SCALE * REPLICA ** 0.5
    master_w1 = jax.random.normal(rng_keys[0], shape_up, jnp.float32) * D ** -0.5
    master_w2 = jax.random.normal(rng_keys[1], shape_down, jnp.float32) * FF ** -0.5
    grad_w1 = jax.random.normal(rng_keys[2], (REPLICA,) + shape_up, jnp.float32) * grad_std
    grad_w2 = jax.random.normal(rng_keys[3], (REPLICA,) + shape_down, jnp.float32) * grad_std
    moment1_w1 = jax.random.normal(rng_keys[4], shape_up, jnp.float32) * (0.2 * GRAD_SCALE)
    moment1_w2 = jax.random.normal(rng_keys[5], shape_down, jnp.float32) * (0.2 * GRAD_SCALE)
    moment2_w1 = (0.1 + 0.2 * jax.random.uniform(rng_keys[6], shape_up, jnp.float32)) * GRAD_SCALE ** 2
    moment2_w2 = (0.1 + 0.2 * jax.random.uniform(rng_keys[7], shape_down, jnp.float32)) * GRAD_SCALE ** 2
    tokens = jax.random.normal(rng_keys[8], (BATCH, D), jnp.float32).astype(jnp.bfloat16)
    base_out = batch_forward(tokens, master_w1.astype(jnp.bfloat16), master_w2.astype(jnp.bfloat16))
    target_noise = jax.random.normal(rng_keys[9], (BATCH, D), jnp.float32)
    targets = (base_out.astype(jnp.float32) + 0.5 * target_noise).astype(jnp.bfloat16)
    return {
        'grad_w1': grad_w1,
        'grad_w2': grad_w2,
        'master_w1': master_w1,
        'master_w2': master_w2,
        'moment1_w1': moment1_w1,
        'moment1_w2': moment1_w2,
        'moment2_w1': moment2_w1,
        'moment2_w2': moment2_w2,
        'tokens': tokens,
        'targets': targets,
    }


def reference(grad_w1, grad_w2, master_w1, master_w2, moment1_w1, moment1_w2, moment2_w1, moment2_w2, tokens, targets):
    new_w1, new_m1, new_v1 = adam_update(grad_w1, master_w1, moment1_w1, moment2_w1)
    new_w2, new_m2, new_v2 = adam_update(grad_w2, master_w2, moment1_w2, moment2_w2)
    full_w1 = new_w1.astype(jnp.bfloat16)
    full_w2 = new_w2.astype(jnp.bfloat16)
    row_loss = batch_loss(tokens, targets, full_w1, full_w2)
    return (row_loss, full_w1, full_w2, new_w1, new_w2, new_m1, new_m2, new_v1, new_v2)
```

```python
import jax
import jax.numpy as jnp
from jax import lax
from jax.experimental import pallas as pl
from jax.experimental.pallas import tpu as pltpu
from jax.sharding import PartitionSpec as P

ADAM_BETA1 = 0.9
ADAM_BETA2 = 0.95
ADAM_EPS = 1e-8
WEIGHT_DECAY = 0.1
STEP = 2
NORM_EPS = 1e-6
LR_COEF = 0.2
GELU_A = 2.0 * (2.0 / jnp.pi) ** 0.5
GELU_B = 8.0 * (2.0 / jnp.pi) ** 0.5 * 0.044715

F32 = jnp.float32
BF16 = jnp.bfloat16
MESH = pl.DeviceIdType.MESH
ROWS = 2048
VMEM_LIMIT = 60 * 1024 * 1024


def adam_shard(grad_mean, master, moment1, moment2, learn_rate):
    new_m = ADAM_BETA1 * moment1 + (1.0 - ADAM_BETA1) * grad_mean
    new_v = ADAM_BETA2 * moment2 + (1.0 - ADAM_BETA2) * grad_mean * grad_mean
    corr_m = 1.0 - ADAM_BETA1 ** STEP
    corr_v = 1.0 - ADAM_BETA2 ** STEP
    step_dir = (new_m / corr_m) / (jnp.sqrt(new_v / corr_v) + ADAM_EPS)
    new_w = master - learn_rate * (step_dir + WEIGHT_DECAY * master)
    return new_w, new_m, new_v


def rms_norm(hidden):
    inv_rms = lax.rsqrt(jnp.mean(hidden * hidden, axis=-1, keepdims=True) + NORM_EPS)
    return (hidden * inv_rms).astype(BF16)


def mlp(normed, hidden, half_up, down):
    half = jnp.dot(normed.astype(F32), half_up, preferred_element_type=F32).astype(BF16).astype(F32)
    act = half * jnp.tanh(half * (GELU_B * (half * half) + GELU_A)) + half
    act = act.astype(BF16).astype(F32)
    return (hidden + jnp.dot(act, down, preferred_element_type=F32)).astype(BF16)


def step_kernel(learn_rate, replicas,
                g1, g2, w1, w2, m1, m2, v1, v2, x,
                h_out, fw1_out, fw2_out, nw1, nw2, nm1, nm2, nv1, nv2,
                g1v, g2v, r1v, r2v, s1, s2, fw1, fw2, xv, nv, up, down,
                sem_g, sem_s, sem_x, sem_out, send_g, recv_g, send_w, recv_w):
    rep, dat = lax.axis_index('replica'), lax.axis_index('data')
    layers = g1.shape[1]
    rows1, rows2 = w1.shape[1], w2.shape[1]
    n_rows = x.shape[0]
    tiles = n_rows // ROWS
    twin = {'replica': 1 - rep}
    peers = [{'data': d} for d in (dat + 1 - 2 * lax.rem(dat, 2), lax.rem(dat + 2, 4), 3 - dat)]

    gcopies = [[pltpu.make_async_copy(g.at[0, l], gv.at[l], sem_g.at[l, k])
                for k, (g, gv) in enumerate(((g1, g1v), (g2, g2v)))] for l in range(layers)]
    for pair in gcopies:
        for c in pair:
            c.start()
    xcopies = [pltpu.make_async_copy(x.at[pl.ds(t * ROWS, ROWS)], xv.at[pl.ds(t * ROWS, ROWS)], sem_x.at[t])
               for t in range(tiles)]
    for c in xcopies:
        c.start()
    scopies = [pltpu.make_async_copy(src, dst.at[i], sem_s.at[k, i])
               for k, (srcs, dst) in enumerate((((w1, m1, v1), s1), ((w2, m2, v2), s2)))
               for i, src in enumerate(srcs)]
    for c in scopies:
        c.start()

    barrier = pltpu.get_barrier_semaphore()
    for dev in [twin] + peers:
        pl.semaphore_signal(barrier, inc=1, device_id=dev, device_id_type=MESH)
    pl.semaphore_wait(barrier, 4)

    gsends = []
    for l in range(layers):
        row = []
        for k, (gv, rv) in enumerate(((g1v, r1v), (g2v, r2v))):
            gcopies[l][k].wait()
            c = pltpu.make_async_remote_copy(
                src_ref=gv.at[l], dst_ref=rv.at[l], send_sem=send_g.at[l, k], recv_sem=recv_g.at[l, k],
                device_id=twin, device_id_type=MESH)
            c.start()
            row.append(c)
        gsends.append(row)

    for t in range(tiles):
        xcopies[t].wait()
        sl = pl.ds(t * ROWS, ROWS)
        nv[sl] = rms_norm(xv[sl].astype(F32))
    for c in scopies:
        c.wait()

    wsends = {}

    def update(l, k):
        gv, rv, s, fw, rows = ((g1v, r1v, s1, fw1, rows1), (g2v, r2v, s2, fw2, rows2))[k]
        gsends[l][k].wait_recv()
        mean = (gv[l] + rv[l]) / replicas
        new_w, new_m, new_v = adam_shard(mean, s[0, l], s[1, l], s[2, l], learn_rate)
        s[0, l], s[1, l], s[2, l] = new_w, new_m, new_v
        mine = pl.ds(pl.multiple_of(dat * rows, rows), rows)
        fw[l, mine] = new_w.astype(BF16)
        out = []
        for j, dev in enumerate(peers):
            c = pltpu.make_async_remote_copy(
                src_ref=fw.at[l, mine], dst_ref=fw.at[l, mine], send_sem=send_w.at[l, k, j],
                recv_sem=recv_w.at[l, k, j], device_id=dev, device_id_type=MESH)
            c.start()
            out.append(c)
        wsends[l, k] = out

    def arrived(l, k):
        for c in wsends[l, k]:
            c.wait_recv()

    update(0, 0)
    update(0, 1)
    update(1, 0)
    arrived(0, 0)
    arrived(0, 1)
    up[...] = fw1[0].astype(F32) * 0.5
    down[...] = fw2[0].astype(F32)
    hcopies = []
    later = {0: ((1, 1),), 1: ((2, 0), (2, 1))}
    for t in range(tiles):
        sl = pl.ds(t * ROWS, ROWS)
        xv[sl] = mlp(nv[sl], xv[sl].astype(F32), up[...], down[...])
        c = pltpu.make_async_copy(xv.at[sl], h_out.at[sl], sem_x.at[t])
        c.start()
        hcopies.append(c)
        for l, k in later.get(t, ()):
            update(l, k)
    outs = [pltpu.make_async_copy(s.at[i], dst, sem_s.at[k, i])
            for k, (s, dsts) in enumerate(((s1, (nw1, nm1, nv1)), (s2, (nw2, nm2, nv2))))
            for i, dst in enumerate(dsts)]
    for c in outs:
        c.start()
    for l in range(1, layers):
        for k in range(2):
            arrived(l, k)
    outs += [pltpu.make_async_copy(fw1, fw1_out, sem_out.at[0]), pltpu.make_async_copy(fw2, fw2_out, sem_out.at[1])]
    for c in outs[-2:]:
        c.start()
    for l in range(layers):
        for k in range(2):
            gsends[l][k].wait_send()
            for c in wsends[l, k]:
                c.wait_send()
    for c in outs + hcopies:
        c.wait()


def tail_kernel(h_in, y, fw1_in, fw2_in, nw1, nw2, nm1, nm2, nv1, nv2,
                loss, fw1_out, fw2_out, ow1, ow2, om1, om2, ov1, ov2,
                hv, yv, fw1, fw2, s1, s2, up, down, sem_h, sem_y, sem_f, sem_s):
    layers = fw1.shape[0]
    tiles = hv.shape[0] // ROWS
    fin = [pltpu.make_async_copy(fw1_in, fw1, sem_f.at[0]), pltpu.make_async_copy(fw2_in, fw2, sem_f.at[1])]
    for c in fin:
        c.start()
    hcs, ycs = [], []
    for t in range(tiles):
        sl = pl.ds(t * ROWS, ROWS)
        hcs.append(pltpu.make_async_copy(h_in.at[sl], hv.at[sl], sem_h.at[t]))
        ycs.append(pltpu.make_async_copy(y.at[sl], yv.at[sl], sem_y.at[t]))
        hcs[-1].start()
        ycs[-1].start()
    sin = [pltpu.make_async_copy(src, dst.at[i], sem_s.at[k, i])
           for k, (srcs, dst) in enumerate((((nw1, nm1, nv1), s1), ((nw2, nm2, nv2), s2)))
           for i, src in enumerate(srcs)]
    for c in sin:
        c.start()
    for c in fin:
        c.wait()
    fout = [pltpu.make_async_copy(fw1, fw1_out, sem_f.at[0]), pltpu.make_async_copy(fw2, fw2_out, sem_f.at[1])]
    for c in fout:
        c.start()
    for l in range(1, layers):
        up[l - 1] = fw1[l].astype(F32) * 0.5
        down[l - 1] = fw2[l].astype(F32)
    for c in sin:
        c.wait()
    sout = [pltpu.make_async_copy(s.at[i], dst, sem_s.at[k, i])
            for k, (s, dsts) in enumerate(((s1, (ow1, om1, ov1)), (s2, (ow2, om2, ov2))))
            for i, dst in enumerate(dsts)]
    for c in sout:
        c.start()

    def tile(t, _):
        sl = pl.ds(pl.multiple_of(t * ROWS, ROWS), ROWS)
        pltpu.make_async_copy(h_in.at[sl], hv.at[sl], sem_h.at[t]).wait()
        hidden = hv[sl]
        for l in range(layers - 1):
            wide = hidden.astype(F32)
            hidden = mlp(rms_norm(wide), wide, up[l], down[l])
        pltpu.make_async_copy(y.at[sl], yv.at[sl], sem_y.at[t]).wait()
        diff = hidden.astype(F32) - yv[sl].astype(F32)
        loss[:, sl] = jnp.mean(diff * diff, axis=-1, keepdims=True).reshape(1, ROWS)
        return 0

    lax.fori_loop(0, tiles, tile, 0)
    for c in fout + sout:
        c.wait()


def solution(mesh):
    replicas = mesh.shape['replica']
    grad_spec = P('replica', None, 'data', None)
    shard_spec = P(None, 'data', None)
    row_spec = P(('replica', 'data'), None)
    loss_spec = P(('replica', 'data'))
    full_spec = P()

    def local_step(g1, g2, w1, w2, m1, m2, v1, v2, tokens, targets):
        learn_rate = LR_COEF * tokens.shape[1] ** -0.5
        n_rows, width = tokens.shape
        layers, rows1, hid = w1.shape
        rows2 = w2.shape[1]
        any_ = pl.BlockSpec(memory_space=pl.ANY)
        full1 = (layers, width, hid)
        full2 = (layers, hid, width)
        tiles = n_rows // ROWS
        sh = jax.ShapeDtypeStruct
        dma = pltpu.SemaphoreType.DMA
        state = [sh(w1.shape, F32), sh(w2.shape, F32)] * 3
        step = pl.pallas_call(
            lambda *refs: step_kernel(learn_rate, replicas, *refs),
            out_shape=[sh((n_rows, width), BF16), sh(full1, BF16), sh(full2, BF16)] + state,
            in_specs=[any_] * 9,
            out_specs=[any_] * 9,
            scratch_shapes=[
                pltpu.VMEM(w1.shape, F32), pltpu.VMEM(w2.shape, F32),
                pltpu.VMEM(w1.shape, F32), pltpu.VMEM(w2.shape, F32),
                pltpu.VMEM((3,) + w1.shape, F32), pltpu.VMEM((3,) + w2.shape, F32),
                pltpu.VMEM(full1, BF16), pltpu.VMEM(full2, BF16),
                pltpu.VMEM((n_rows, width), BF16), pltpu.VMEM((n_rows, width), BF16),
                pltpu.VMEM((width, hid), F32), pltpu.VMEM((hid, width), F32),
                dma((layers, 2)), dma((2, 3)), dma((tiles,)), dma((2,)),
                dma((layers, 2)), dma((layers, 2)), dma((layers, 2, 3)), dma((layers, 2, 3)),
            ],
            compiler_params=pltpu.CompilerParams(
                collective_id=0, has_side_effects=True, vmem_limit_bytes=VMEM_LIMIT),
            name='step',
        )
        mid = step(g1, g2, w1, w2, m1, m2, v1, v2, tokens)
        tail = pl.pallas_call(
            tail_kernel,
            out_shape=[sh((1, n_rows), F32), sh(full1, BF16), sh(full2, BF16)] + state,
            in_specs=[any_] * 10,
            out_specs=[pl.BlockSpec(memory_space=pltpu.VMEM)] + [any_] * 8,
            scratch_shapes=[
                pltpu.VMEM((n_rows, width), BF16), pltpu.VMEM((n_rows, width), BF16),
                pltpu.VMEM(full1, BF16), pltpu.VMEM(full2, BF16),
                pltpu.VMEM((3,) + w1.shape, F32), pltpu.VMEM((3,) + w2.shape, F32),
                pltpu.VMEM((layers - 1, width, hid), F32), pltpu.VMEM((layers - 1, hid, width), F32),
                dma((tiles,)), dma((tiles,)), dma((2,)), dma((2, 3)),
            ],
            compiler_params=pltpu.CompilerParams(vmem_limit_bytes=VMEM_LIMIT),
            name='tail',
        )
        outs = tail(mid[0], targets, *mid[1:])
        return (outs[0].reshape(n_rows),) + tuple(outs[1:])

    return jax.shard_map(
        local_step,
        mesh=mesh,
        in_specs=(grad_spec, grad_spec, shard_spec, shard_spec, shard_spec, shard_spec, shard_spec, shard_spec, row_spec, row_spec),
        out_specs=(loss_spec, full_spec, full_spec, shard_spec, shard_spec, shard_spec, shard_spec, shard_spec, shard_spec),
        check_vma=False,
    )
```

```python
import jax
import jax.numpy as jnp
from jax import lax
from jax.experimental import pallas as pl
from jax.experimental.pallas import tpu as pltpu
from jax.sharding import PartitionSpec as P

ADAM_BETA1 = 0.9
ADAM_BETA2 = 0.95
ADAM_EPS = 1e-8
WEIGHT_DECAY = 0.1
STEP = 2
NORM_EPS = 1e-6
LR_COEF = 0.2
GELU_A = 2.0 * (2.0 / jnp.pi) ** 0.5
GELU_B = 8.0 * (2.0 / jnp.pi) ** 0.5 * 0.044715

F32 = jnp.float32
BF16 = jnp.bfloat16
MESH = pl.DeviceIdType.MESH
ROWS = 2048
VMEM_LIMIT = 44 * 1024 * 1024


def adam_shard(grad_mean, master, moment1, moment2, learn_rate):
    new_m = ADAM_BETA1 * moment1 + (1.0 - ADAM_BETA1) * grad_mean
    new_v = ADAM_BETA2 * moment2 + (1.0 - ADAM_BETA2) * grad_mean * grad_mean
    corr_m = 1.0 - ADAM_BETA1 ** STEP
    corr_v = 1.0 - ADAM_BETA2 ** STEP
    step_dir = (new_m / corr_m) / (jnp.sqrt(new_v / corr_v) + ADAM_EPS)
    new_w = master - learn_rate * (step_dir + WEIGHT_DECAY * master)
    return new_w, new_m, new_v


def rms_norm(hidden):
    inv_rms = lax.rsqrt(jnp.mean(hidden * hidden, axis=-1, keepdims=True) + NORM_EPS)
    return (hidden * inv_rms).astype(BF16)


def mlp_up(normed, half_up):
    half = jnp.dot(normed.astype(F32), half_up, preferred_element_type=F32).astype(BF16).astype(F32)
    act = half * jnp.tanh(half * (GELU_B * (half * half) + GELU_A)) + half
    return act.astype(BF16)


def mlp_down(act, hidden, down):
    return (hidden + jnp.dot(act.astype(F32), down, preferred_element_type=F32)).astype(BF16)


def step_kernel(learn_rate, replicas,
                g1, g2, w1, w2, m1, m2, v1, v2, x,
                h_out, fw1, fw2, s1, s2,
                g1v, g2v, r1v, r2v, xv, nv, av, up, down,
                sem_g, sem_s, sem_x, send_g, recv_g, send_w, recv_w):
    rep, dat = lax.axis_index('replica'), lax.axis_index('data')
    layers = g1.shape[1]
    rows1, rows2 = w1.shape[1], w2.shape[1]
    tiles = x.shape[0] // ROWS
    sls = [pl.ds(t * ROWS, ROWS) for t in range(tiles)]
    twin = {'replica': 1 - rep}
    peers = [{'data': d} for d in (dat + 1 - 2 * lax.rem(dat, 2), lax.rem(dat + 2, 4), 3 - dat)]

    gcopies = [[pltpu.make_async_copy(g.at[0, l], gv.at[l], sem_g.at[l, k])
                for k, (g, gv) in enumerate(((g1, g1v), (g2, g2v)))] for l in range(layers)]
    for pair in gcopies:
        for c in pair:
            c.start()

    barrier = pltpu.get_barrier_semaphore()
    for dev in [twin] + peers:
        pl.semaphore_signal(barrier, inc=1, device_id=dev, device_id_type=MESH)
    with jax.named_scope('barrier'):
        pl.semaphore_wait(barrier, 4)

    half_cols = w1.shape[2] // 2
    pieces = [(0, 0, pl.ds(0, half_cols)), (0, 0, pl.ds(half_cols, half_cols)), (0, 1, slice(None))]
    pieces += [(l, k, slice(None)) for l in range(1, layers) for k in range(2)]
    gsends = []
    with jax.named_scope('gsend'):
        for p, (l, k, cols) in enumerate(pieces):
            gv, rv = ((g1v, r1v), (g2v, r2v))[k]
            if p != 1:
                gcopies[l][k].wait()
            c = pltpu.make_async_remote_copy(
                src_ref=gv.at[l, :, cols], dst_ref=rv.at[l, :, cols], send_sem=send_g.at[p], recv_sem=recv_g.at[p],
                device_id=twin, device_id_type=MESH)
            c.start()
            gsends.append(c)

    xcopies = [pltpu.make_async_copy(x.at[sl], xv.at[sl], sem_x.at[t]) for t, sl in enumerate(sls)]
    scopies = [pltpu.make_async_copy(src, dst.at[i], sem_s.at[k, i])
               for k, (srcs, dst) in enumerate((((w1, m1, v1), s1), ((w2, m2, v2), s2)))
               for i, src in enumerate(srcs)]
    for c in xcopies + scopies:
        c.start()
    for t, sl in enumerate(sls):
        with jax.named_scope('norm'):
            xcopies[t].wait()
            nv[sl] = rms_norm(xv[sl].astype(F32))
    for c in scopies:
        c.wait()

    wsends = []

    def update(p):
        l, k, cols = pieces[p]
        gv, rv, s, fw, rows = ((g1v, r1v, s1, fw1, rows1), (g2v, r2v, s2, fw2, rows2))[k]
        with jax.named_scope(f'waitg{p}'):
            gsends[p].wait_recv()
        mean = (gv[l, :, cols] + rv[l, :, cols]) / replicas
        new = adam_shard(mean, s[0, l, :, cols], s[1, l, :, cols], s[2, l, :, cols], learn_rate)
        for i in range(3):
            s[i, l, :, cols] = new[i]
        mine = pl.ds(pl.multiple_of(dat * rows, rows), rows)
        fw[l, mine, cols] = new[0].astype(BF16)
        out = []
        for j, dev in enumerate(peers):
            c = pltpu.make_async_remote_copy(
                src_ref=fw.at[l, mine, cols], dst_ref=fw.at[l, mine, cols], send_sem=send_w.at[p, j],
                recv_sem=recv_w.at[p, j], device_id=dev, device_id_type=MESH)
            c.start()
            out.append(c)
        wsends.append(out)

    def arrived(p):
        with jax.named_scope(f'waitw{p}'):
            for c in wsends[p]:
                c.wait_recv()

    def layer(l, ts):
        with jax.named_scope(f'layer{l}'):
            for t in ts:
                wide = xv[sls[t]].astype(F32)
                normed = nv[sls[t]] if l == 0 else rms_norm(wide)
                dst = h_out if l == 1 else xv
                dst[sls[t]] = mlp_down(mlp_up(normed, up[...]), wide, down[...])

    update(0)
    update(1)
    for p in range(2):
        arrived(p)
        cols = pieces[p][2]
        with jax.named_scope(f'up{p}'):
            up[:, cols] = fw1[0, :, cols].astype(F32) * 0.5
            av[sls[0], cols] = mlp_up(nv[sls[0]], up[:, cols])
        if p == 0:
            update(2)
    update(3)
    with jax.named_scope('up'):
        av[sls[1]] = mlp_up(nv[sls[1]], up[...])
    arrived(2)
    down[...] = fw2[0].astype(F32)
    update(4)
    with jax.named_scope('layer0'):
        for sl in sls[:2]:
            xv[sl] = mlp_down(av[sl], xv[sl].astype(F32), down[...])
        layer(0, range(2, tiles))
    update(5)
    update(6)
    arrived(3)
    arrived(4)
    up[...] = fw1[1].astype(F32) * 0.5
    down[...] = fw2[1].astype(F32)
    layer(1, range(tiles))
    arrived(5)
    arrived(6)
    with jax.named_scope('waitsend'):
        for c in gsends + [c for out in wsends for c in out]:
            c.wait_send()


def tail_kernel(h, fw1, fw2, s1, s2, y,
                loss, fw1_out, fw2_out, ow1, ow2, om1, om2, ov1, ov2,
                up, down, sem_f, sem_s):
    last = fw1.shape[0] - 1
    tiles = h.shape[0] // ROWS
    sls = [pl.ds(t * ROWS, ROWS) for t in range(tiles)]
    outs = [pltpu.make_async_copy(s.at[i], dst, sem_s.at[k, i])
            for k, (s, dsts) in enumerate(((s1, (ow1, om1, ov1)), (s2, (ow2, om2, ov2))))
            for i, dst in enumerate(dsts)]
    outs += [pltpu.make_async_copy(fw1, fw1_out, sem_f.at[0]), pltpu.make_async_copy(fw2, fw2_out, sem_f.at[1])]
    for c in outs:
        c.start()
    up[...] = fw1[last].astype(F32) * 0.5
    down[...] = fw2[last].astype(F32)
    with jax.named_scope('last'):
        for sl in sls:
            wide = h[sl].astype(F32)
            hidden = mlp_down(mlp_up(rms_norm(wide), up[...]), wide, down[...])
            diff = hidden.astype(F32) - y[sl].astype(F32)
            loss[:, sl] = jnp.mean(diff * diff, axis=-1, keepdims=True).reshape(1, ROWS)
    with jax.named_scope('waitout'):
        for c in outs:
            c.wait()


def solution(mesh):
    replicas = mesh.shape['replica']
    grad_spec = P('replica', None, 'data', None)
    shard_spec = P(None, 'data', None)
    row_spec = P(('replica', 'data'), None)
    loss_spec = P(('replica', 'data'))
    full_spec = P()

    def local_step(g1, g2, w1, w2, m1, m2, v1, v2, tokens, targets):
        learn_rate = LR_COEF * tokens.shape[1] ** -0.5
        n_rows, width = tokens.shape
        layers, rows1, hid = w1.shape
        rows2 = w2.shape[1]
        any_ = pl.BlockSpec(memory_space=pl.ANY)
        full1 = (layers, width, hid)
        full2 = (layers, hid, width)
        tiles = n_rows // ROWS
        pieces = 2 * layers + 1
        sh = jax.ShapeDtypeStruct
        dma = pltpu.SemaphoreType.DMA
        vmem = pl.BlockSpec(memory_space=pltpu.VMEM)
        step = pl.pallas_call(
            lambda *refs: step_kernel(learn_rate, replicas, *refs),
            out_shape=[pltpu.VMEM((n_rows, width), BF16), pltpu.VMEM(full1, BF16), pltpu.VMEM(full2, BF16),
                       pltpu.VMEM((3,) + w1.shape, F32), pltpu.VMEM((3,) + w2.shape, F32)],
            in_specs=[any_] * 9,
            out_specs=[vmem] * 5,
            scratch_shapes=[
                pltpu.VMEM(w1.shape, F32), pltpu.VMEM(w2.shape, F32),
                pltpu.VMEM(w1.shape, F32), pltpu.VMEM(w2.shape, F32),
                pltpu.VMEM((n_rows, width), BF16), pltpu.VMEM((n_rows, width), BF16),
                pltpu.VMEM((2 * ROWS, hid), BF16),
                pltpu.VMEM((width, hid), F32), pltpu.VMEM((hid, width), F32),
                dma((layers, 2)), dma((2, 3)), dma((tiles,)),
                dma((pieces,)), dma((pieces,)), dma((pieces, 3)), dma((pieces, 3)),
            ],
            compiler_params=pltpu.CompilerParams(
                collective_id=0, has_side_effects=True, vmem_limit_bytes=VMEM_LIMIT),
            name='step',
        )
        mid = step(*(pltpu.with_memory_space_constraint(a, pltpu.HBM)
                     for a in (g1, g2, w1, w2, m1, m2, v1, v2, tokens)))
        mid = [pltpu.with_memory_space_constraint(a, pltpu.VMEM) for a in mid]
        tail = pl.pallas_call(
            tail_kernel,
            out_shape=[sh((1, n_rows), F32), sh(full1, BF16), sh(full2, BF16)]
            + [sh(w1.shape, F32), sh(w2.shape, F32)] * 3,
            in_specs=[vmem] * 6,
            out_specs=[vmem] + [any_] * 8,
            scratch_shapes=[
                pltpu.VMEM((width, hid), F32), pltpu.VMEM((hid, width), F32),
                dma((2,)), dma((2, 3)),
            ],
            compiler_params=pltpu.CompilerParams(vmem_limit_bytes=VMEM_LIMIT),
            name='tail',
        )
        outs = tail(*mid, targets)
        return (outs[0].reshape(n_rows),) + tuple(outs[1:])

    return jax.shard_map(
        local_step,
        mesh=mesh,
        in_specs=(grad_spec, grad_spec, shard_spec, shard_spec, shard_spec, shard_spec, shard_spec, shard_spec, row_spec, row_spec),
        out_specs=(loss_spec, full_spec, full_spec, shard_spec, shard_spec, shard_spec, shard_spec, shard_spec, shard_spec),
        check_vma=False,
    )
```

```python
import jax
import jax.numpy as jnp
from jax import lax
from jax.experimental import pallas as pl
from jax.experimental.pallas import tpu as pltpu
from jax.sharding import PartitionSpec as P

ADAM_BETA1 = 0.9
ADAM_BETA2 = 0.95
ADAM_EPS = 1e-8
WEIGHT_DECAY = 0.1
STEP = 2
NORM_EPS = 1e-6
LR_COEF = 0.2
GELU_A = 2.0 * (2.0 / jnp.pi) ** 0.5
GELU_B = 8.0 * (2.0 / jnp.pi) ** 0.5 * 0.044715

F32 = jnp.float32
BF16 = jnp.bfloat16
MESH = pl.DeviceIdType.MESH
ROWS = 2048
PIECE_ROWS = 4096
EARLY_ROWS = 4096
MID_ROWS = 6144
CUTS = 4
VMEM_LIMIT = 44 * 1024 * 1024


def adam_shard(grad_mean, master, moment1, moment2, learn_rate):
    new_m = ADAM_BETA1 * moment1 + (1.0 - ADAM_BETA1) * grad_mean
    new_v = ADAM_BETA2 * moment2 + (1.0 - ADAM_BETA2) * grad_mean * grad_mean
    corr_m = 1.0 - ADAM_BETA1 ** STEP
    corr_v = 1.0 - ADAM_BETA2 ** STEP
    step_dir = (new_m / corr_m) / (jnp.sqrt(new_v / corr_v) + ADAM_EPS)
    new_w = master - learn_rate * (step_dir + WEIGHT_DECAY * master)
    return new_w, new_m, new_v


def rms_norm(hidden):
    inv_rms = lax.rsqrt(jnp.mean(hidden * hidden, axis=-1, keepdims=True) + NORM_EPS)
    return (hidden * inv_rms).astype(BF16)


def row_mean_sq(rows):
    return jnp.sum((rows * rows).T, axis=0, keepdims=True) * (1.0 / rows.shape[1])


def rms_norm_t(hidden):
    inv_rms = lax.rsqrt(row_mean_sq(hidden) + NORM_EPS)
    return (hidden * jnp.broadcast_to(inv_rms, hidden.shape[::-1]).T).astype(BF16)


def mlp_up(normed, half_up):
    half = jnp.dot(normed, half_up, preferred_element_type=F32).astype(BF16).astype(F32)
    return half * jnp.tanh(half * (GELU_B * (half * half) + GELU_A)) + half


def mlp_down(act, hidden, down):
    return (hidden + jnp.dot(act, down, preferred_element_type=F32)).astype(BF16)


def step_kernel(learn_rate, replicas,
                g1, g2, w1, w2, m1, m2, v1, v2, x,
                h_out, n_out, fw1, fw2, s1, s2,
                g1v, g2v, r1v, r2v, xv, nv, av, up, down,
                sem_g, sem_s, sem_x, send_g, recv_g, send_w, recv_w):
    rep, dat = lax.axis_index('replica'), lax.axis_index('data')
    layers = g1.shape[1]
    rows1, rows2 = w1.shape[1], w2.shape[1]
    tiles = x.shape[0] // ROWS
    sls = [pl.ds(t * ROWS, ROWS) for t in range(tiles)]
    twin = {'replica': 1 - rep}
    peers = [{'data': d} for d in (dat + 1 - 2 * lax.rem(dat, 2), lax.rem(dat + 2, 4), 3 - dat)]

    gcopies = [[pltpu.make_async_copy(g.at[0, l], gv.at[l], sem_g.at[l, k])
                for k, (g, gv) in enumerate(((g1, g1v), (g2, g2v)))] for l in range(layers)]
    for pair in gcopies:
        for c in pair:
            c.start()

    barrier = pltpu.get_barrier_semaphore()
    for dev in [twin] + peers:
        pl.semaphore_signal(barrier, inc=1, device_id=dev, device_id_type=MESH)
    with jax.named_scope('barrier'):
        pl.semaphore_wait(barrier, 4)

    cut = w1.shape[2] // CUTS
    pieces = [(0, 0, pl.ds(i * cut, cut)) for i in range(CUTS)] + [(0, 1, slice(None))]
    pieces += [(l, k, slice(None)) for l in range(1, layers) for k in range(2)]
    gsends = []
    with jax.named_scope('gsend'):
        for p, (l, k, cols) in enumerate(pieces):
            gv, rv = ((g1v, r1v), (g2v, r2v))[k]
            if p not in range(1, CUTS):
                gcopies[l][k].wait()
            c = pltpu.make_async_remote_copy(
                src_ref=gv.at[l, :, cols], dst_ref=rv.at[l, :, cols], send_sem=send_g.at[p], recv_sem=recv_g.at[p],
                device_id=twin, device_id_type=MESH)
            c.start()
            gsends.append(c)

    xcopies = [pltpu.make_async_copy(x.at[sl], xv.at[sl], sem_x.at[t]) for t, sl in enumerate(sls)]
    scopies = [pltpu.make_async_copy(src, dst.at[i], sem_s.at[k, i])
               for k, (srcs, dst) in enumerate((((w1, m1, v1), s1), ((w2, m2, v2), s2)))
               for i, src in enumerate(srcs)]
    for c in xcopies + scopies:
        c.start()
    for t, sl in enumerate(sls):
        with jax.named_scope('norm'):
            xcopies[t].wait()
            nv[sl] = rms_norm(xv[sl].astype(F32))
    for c in scopies:
        c.wait()

    wsends = []

    def update(p):
        l, k, cols = pieces[p]
        gv, rv, s, fw, rows = ((g1v, r1v, s1, fw1, rows1), (g2v, r2v, s2, fw2, rows2))[k]
        with jax.named_scope(f'waitg{p}'):
            gsends[p].wait_recv()
        mean = (gv[l, :, cols] + rv[l, :, cols]) / replicas
        new = adam_shard(mean, s[0, l, :, cols], s[1, l, :, cols], s[2, l, :, cols], learn_rate)
        for i in range(3):
            s[i, l, :, cols] = new[i]
        mine = pl.ds(pl.multiple_of(dat * rows, rows), rows)
        fw[l, mine, cols] = new[0].astype(BF16)
        out = []
        for j, dev in enumerate(peers):
            c = pltpu.make_async_remote_copy(
                src_ref=fw.at[l, mine, cols], dst_ref=fw.at[l, mine, cols], send_sem=send_w.at[p, j],
                recv_sem=recv_w.at[p, j], device_id=dev, device_id_type=MESH)
            c.start()
            out.append(c)
        wsends.append(out)

    def arrived(p):
        with jax.named_scope(f'waitw{p}'):
            for c in wsends[p]:
                c.wait_recv()

    n_rows = x.shape[0]

    def finish(sl, act, h_ref, n_ref):
        hidden = mlp_down(act, xv[sl].astype(F32), down[...])
        h_ref[sl] = hidden
        n_ref[sl] = rms_norm_t(hidden.astype(F32))

    for p in range(CUTS + 1):
        update(p)
    early = pl.ds(0, PIECE_ROWS)
    for p in range(CUTS):
        arrived(p)
        cols = pieces[p][2]
        with jax.named_scope(f'up{p}'):
            up[:, cols] = fw1[0, :, cols] * 0.5
            av[early, cols] = mlp_up(nv[early], up[:, cols])
        if p == 1:
            update(CUTS + 1)
    if EARLY_ROWS > PIECE_ROWS:
        with jax.named_scope('up'):
            sl = pl.ds(PIECE_ROWS, EARLY_ROWS - PIECE_ROWS)
            av[sl] = mlp_up(nv[sl], up[...])
    arrived(CUTS)
    down[...] = fw2[0].astype(F32)
    update(CUTS + 2)
    with jax.named_scope('layer0'):
        sl = pl.ds(0, EARLY_ROWS)
        finish(sl, av[sl], xv, nv)
        sl = pl.ds(EARLY_ROWS, MID_ROWS - EARLY_ROWS)
        finish(sl, mlp_up(nv[sl], up[...]), xv, nv)
    update(CUTS + 3)
    update(CUTS + 4)
    arrived(CUTS + 1)
    arrived(CUTS + 2)
    with jax.named_scope('layer1'):
        if n_rows > MID_ROWS:
            sl = pl.ds(MID_ROWS, n_rows - MID_ROWS)
            finish(sl, mlp_up(nv[sl], up[...]), xv, nv)
        up[...] = fw1[1] * 0.5
        down[...] = fw2[1].astype(F32)
        sl = pl.ds(0, n_rows)
        finish(sl, mlp_up(nv[sl], up[...]), h_out, n_out)
    arrived(CUTS + 3)
    arrived(CUTS + 4)
    with jax.named_scope('waitsend'):
        for c in gsends + [c for out in wsends for c in out]:
            c.wait_send()


def tail_kernel(h, n, fw1, fw2, s1, s2, y,
                loss, fw1_out, fw2_out, ow1, ow2, om1, om2, ov1, ov2,
                up, down, sem_f, sem_s):
    last = fw1.shape[0] - 1
    outs = [pltpu.make_async_copy(s.at[i], dst, sem_s.at[k, i])
            for k, (s, dsts) in enumerate(((s1, (ow1, om1, ov1)), (s2, (ow2, om2, ov2))))
            for i, dst in enumerate(dsts)]
    outs += [pltpu.make_async_copy(fw1, fw1_out, sem_f.at[0]), pltpu.make_async_copy(fw2, fw2_out, sem_f.at[1])]
    for c in outs:
        c.start()
    with jax.named_scope('last'):
        up[...] = fw1[last] * 0.5
        down[...] = fw2[last].astype(F32)
        hidden = mlp_down(mlp_up(n[...], up[...]), h[...].astype(F32), down[...])
        loss[...] = row_mean_sq(hidden.astype(F32) - y[...].astype(F32))
    with jax.named_scope('waitout'):
        for c in outs:
            c.wait()


def solution(mesh):
    replicas = mesh.shape['replica']
    grad_spec = P('replica', None, 'data', None)
    shard_spec = P(None, 'data', None)
    row_spec = P(('replica', 'data'), None)
    loss_spec = P(('replica', 'data'))
    full_spec = P()

    def local_step(g1, g2, w1, w2, m1, m2, v1, v2, tokens, targets):
        learn_rate = LR_COEF * tokens.shape[1] ** -0.5
        n_rows, width = tokens.shape
        layers, rows1, hid = w1.shape
        rows2 = w2.shape[1]
        any_ = pl.BlockSpec(memory_space=pl.ANY)
        full1 = (layers, width, hid)
        full2 = (layers, hid, width)
        tiles = n_rows // ROWS
        pieces = 2 * layers - 1 + CUTS
        sh = jax.ShapeDtypeStruct
        dma = pltpu.SemaphoreType.DMA
        vmem = pl.BlockSpec(memory_space=pltpu.VMEM)
        step = pl.pallas_call(
            lambda *refs: step_kernel(learn_rate, replicas, *refs),
            out_shape=[pltpu.VMEM((n_rows, width), BF16), pltpu.VMEM((n_rows, width), BF16), pltpu.VMEM(full1, BF16), pltpu.VMEM(full2, BF16),
                       pltpu.VMEM((3,) + w1.shape, F32), pltpu.VMEM((3,) + w2.shape, F32)],
            in_specs=[any_] * 9,
            out_specs=[vmem] * 6,
            scratch_shapes=[
                pltpu.VMEM(w1.shape, F32), pltpu.VMEM(w2.shape, F32),
                pltpu.VMEM(w1.shape, F32), pltpu.VMEM(w2.shape, F32),
                pltpu.VMEM((n_rows, width), BF16), pltpu.VMEM((n_rows, width), BF16),
                pltpu.VMEM((EARLY_ROWS, hid), F32),
                pltpu.VMEM((width, hid), BF16), pltpu.VMEM((hid, width), F32),
                dma((layers, 2)), dma((2, 3)), dma((tiles,)),
                dma((pieces,)), dma((pieces,)), dma((pieces, 3)), dma((pieces, 3)),
            ],
            compiler_params=pltpu.CompilerParams(
                collective_id=0, has_side_effects=True, vmem_limit_bytes=VMEM_LIMIT),
            name='step',
        )
        mid = step(*(pltpu.with_memory_space_constraint(a, pltpu.HBM)
                     for a in (g1, g2, w1, w2, m1, m2, v1, v2, tokens)))
        mid = [pltpu.with_memory_space_constraint(a, pltpu.VMEM) for a in mid]
        tail = pl.pallas_call(
            tail_kernel,
            out_shape=[sh((1, n_rows), F32), sh(full1, BF16), sh(full2, BF16)]
            + [sh(w1.shape, F32), sh(w2.shape, F32)] * 3,
            in_specs=[vmem] * 7,
            out_specs=[vmem] + [any_] * 8,
            scratch_shapes=[
                pltpu.VMEM((width, hid), BF16), pltpu.VMEM((hid, width), F32),
                dma((2,)), dma((2, 3)),
            ],
            compiler_params=pltpu.CompilerParams(vmem_limit_bytes=VMEM_LIMIT),
            name='tail',
        )
        outs = tail(*mid, targets)
        return (outs[0].reshape(n_rows),) + tuple(outs[1:])

    return jax.shard_map(
        local_step,
        mesh=mesh,
        in_specs=(grad_spec, grad_spec, shard_spec, shard_spec, shard_spec, shard_spec, shard_spec, shard_spec, row_spec, row_spec),
        out_specs=(loss_spec, full_spec, full_spec, shard_spec, shard_spec, shard_spec, shard_spec, shard_spec, shard_spec),
        check_vma=False,
    )
```

```python
import jax
import jax.numpy as jnp
from jax import lax
from jax.experimental import pallas as pl
from jax.experimental.pallas import tpu as pltpu
from jax.sharding import PartitionSpec as P

ADAM_BETA1 = 0.9
ADAM_BETA2 = 0.95
ADAM_EPS = 1e-8
WEIGHT_DECAY = 0.1
STEP = 2
NORM_EPS = 1e-6
LR_COEF = 0.2
GELU_A = 2.0 * (2.0 / jnp.pi) ** 0.5
GELU_B = 8.0 * (2.0 / jnp.pi) ** 0.5 * 0.044715

F32 = jnp.float32
BF16 = jnp.bfloat16
MESH = pl.DeviceIdType.MESH
ROWS = 2048
PIECE_ROWS = 4096
EARLY_ROWS = 4096
MID_ROWS = 6144
CUTS = 4
VMEM_LIMIT = 44 * 1024 * 1024


def adam_shard(grad_mean, master, moment1, moment2, learn_rate):
    new_m = ADAM_BETA1 * moment1 + (1.0 - ADAM_BETA1) * grad_mean
    new_v = ADAM_BETA2 * moment2 + (1.0 - ADAM_BETA2) * grad_mean * grad_mean
    corr_m = 1.0 - ADAM_BETA1 ** STEP
    corr_v = 1.0 - ADAM_BETA2 ** STEP
    step_dir = (new_m / corr_m) / (jnp.sqrt(new_v / corr_v) + ADAM_EPS)
    new_w = master - learn_rate * (step_dir + WEIGHT_DECAY * master)
    return new_w, new_m, new_v


def rms_norm(hidden):
    inv_rms = lax.rsqrt(jnp.mean(hidden * hidden, axis=-1, keepdims=True) + NORM_EPS)
    return (hidden * inv_rms).astype(BF16)


def row_mean_sq(rows):
    return jnp.sum((rows * rows).T, axis=0, keepdims=True) * (1.0 / rows.shape[1])


def rms_norm_t(hidden):
    cols = hidden.T.astype(F32)
    inv_rms = lax.rsqrt(jnp.sum(cols * cols, axis=0, keepdims=True) * (1.0 / cols.shape[0]) + NORM_EPS)
    return (cols * inv_rms).astype(BF16).T


def mlp_up(normed, half_up):
    half = jnp.dot(normed, half_up, preferred_element_type=F32).astype(BF16).astype(F32)
    return half * jnp.tanh(half * (GELU_B * (half * half) + GELU_A)) + half


def mlp_down(act, hidden, down):
    return (hidden + jnp.dot(act, down, preferred_element_type=F32)).astype(BF16)


def wait_bytes(ref, sem):
    pltpu.make_async_copy(ref, ref, sem).wait()


def step_kernel(learn_rate, replicas,
                g1, g2, w1, w2, m1, m2, v1, v2, x,
                h_out, n_out, fw1, fw2, s1, s2,
                g1v, g2v, r1v, r2v, xv, nv, av, up, down,
                sem_g, sem_s, sem_x, send_g, recv_g, send_w, recv_w):
    rep, dat = lax.axis_index('replica'), lax.axis_index('data')
    layers = g1.shape[1]
    rows1, rows2 = w1.shape[1], w2.shape[1]
    tiles = x.shape[0] // ROWS
    sls = [pl.ds(t * ROWS, ROWS) for t in range(tiles)]
    twin = {'replica': 1 - rep}
    peers = [{'data': d} for d in (dat + 1 - 2 * lax.rem(dat, 2), lax.rem(dat + 2, 4), 3 - dat)]

    gcopies = [pltpu.make_async_copy(g1.at[0, 0], g1v.at[0], sem_g.at[0]),
               pltpu.make_async_copy(g2.at[0], g2v, sem_g.at[1]),
               pltpu.make_async_copy(g1.at[0, pl.ds(1, layers - 1)], g1v.at[pl.ds(1, layers - 1)], sem_g.at[2])]
    for c in gcopies:
        c.start()

    barrier = pltpu.get_barrier_semaphore()
    for dev in [twin] + peers:
        pl.semaphore_signal(barrier, inc=1, device_id=dev, device_id_type=MESH)
    with jax.named_scope('barrier'):
        pl.semaphore_wait(barrier, 4)

    cut = w1.shape[2] // CUTS
    pieces = [(0, 0, pl.ds(i * cut, cut)) for i in range(CUTS)] + [(0, 1, slice(None))]
    pieces += [(l, k, slice(None)) for l in range(1, layers) for k in range(2)]
    gsends = []
    with jax.named_scope('gsend'):
        for p, (l, k, cols) in enumerate(pieces):
            gv, rv = ((g1v, r1v), (g2v, r2v))[k]
            if p in (0, CUTS, CUTS + 1):
                gcopies[(0, CUTS, CUTS + 1).index(p)].wait()
            c = pltpu.make_async_remote_copy(
                src_ref=gv.at[l, :, cols], dst_ref=rv.at[l, :, cols], send_sem=send_g, recv_sem=recv_g.at[p],
                device_id=twin, device_id_type=MESH)
            c.start()
            gsends.append(c)

    mid = x.shape[0] // 2
    xcopies = [pltpu.make_async_copy(x.at[sl], xv.at[sl], sem_x.at[t]) for t, sl in enumerate((pl.ds(0, mid), pl.ds(mid, mid)))]
    scopies = [pltpu.make_async_copy(src, dst.at[i], sem_s)
               for srcs, dst in (((w1, m1, v1), s1), ((w2, m2, v2), s2)) for i, src in enumerate(srcs)]
    for c in xcopies + scopies:
        c.start()
    for t, sl in enumerate(sls):
        with jax.named_scope('norm'):
            if t % (tiles // 2) == 0:
                xcopies[t // (tiles // 2)].wait()
            nv[sl] = rms_norm(xv[sl].astype(F32))
    row_bytes = av.shape[1] * 4
    wait_bytes(av.at[pl.ds(0, 3 * (w1.size + w2.size) * 4 // row_bytes)], sem_s)

    def update(p):
        l, k, cols = pieces[p]
        gv, rv, s, fw, rows = ((g1v, r1v, s1, fw1, rows1), (g2v, r2v, s2, fw2, rows2))[k]
        with jax.named_scope(f'waitg{p}'):
            gsends[p].wait_recv()
        mean = (gv[l, :, cols] + rv[l, :, cols]) / replicas
        new = adam_shard(mean, s[0, l, :, cols], s[1, l, :, cols], s[2, l, :, cols], learn_rate)
        for i in range(3):
            s[i, l, :, cols] = new[i]
        mine = pl.ds(pl.multiple_of(dat * rows, rows), rows)
        fw[l, mine, cols] = new[0].astype(BF16)
        for dev in peers:
            pltpu.make_async_remote_copy(
                src_ref=fw.at[l, mine, cols], dst_ref=fw.at[l, mine, cols], send_sem=send_w,
                recv_sem=recv_w.at[p], device_id=dev, device_id_type=MESH).start()

    def arrived(p):
        l, k, cols = pieces[p]
        fw, rows = ((fw1, rows1), (fw2, rows2))[k]
        with jax.named_scope(f'waitw{p}'):
            wait_bytes(fw.at[l, pl.ds(0, len(peers) * rows), cols], recv_w.at[p])

    n_rows = x.shape[0]

    def finish(sl, act, h_ref, n_ref):
        hidden = mlp_down(act, xv[sl].astype(F32), down[...])
        h_ref[sl] = hidden
        n_ref[sl] = rms_norm(hidden.astype(F32))

    for p in range(CUTS + 1):
        update(p)
    early = pl.ds(0, PIECE_ROWS)
    for p in range(CUTS):
        arrived(p)
        cols = pieces[p][2]
        with jax.named_scope(f'up{p}'):
            up[:, cols] = fw1[0, :, cols] * 0.5
            av[early, cols] = mlp_up(nv[early], up[:, cols])
        if p == 1:
            update(CUTS + 1)
    if EARLY_ROWS > PIECE_ROWS:
        with jax.named_scope('up'):
            sl = pl.ds(PIECE_ROWS, EARLY_ROWS - PIECE_ROWS)
            av[sl] = mlp_up(nv[sl], up[...])
    arrived(CUTS)
    down[...] = fw2[0].astype(F32)
    update(CUTS + 2)
    with jax.named_scope('layer0'):
        sl = pl.ds(0, EARLY_ROWS)
        finish(sl, av[sl], xv, nv)
        sl = pl.ds(EARLY_ROWS, MID_ROWS - EARLY_ROWS)
        finish(sl, mlp_up(nv[sl], up[...]), xv, nv)
    update(CUTS + 3)
    update(CUTS + 4)
    arrived(CUTS + 1)
    arrived(CUTS + 2)
    with jax.named_scope('layer1'):
        if n_rows > MID_ROWS:
            sl = pl.ds(MID_ROWS, n_rows - MID_ROWS)
            finish(sl, mlp_up(nv[sl], up[...]), xv, nv)
        up[...] = fw1[1] * 0.5
        down[...] = fw2[1].astype(F32)
        sl = pl.ds(0, n_rows)
        finish(sl, mlp_up(nv[sl], up[...]), h_out, n_out)
    arrived(CUTS + 3)
    arrived(CUTS + 4)
    with jax.named_scope('waitsend'):
        wait_bytes(av.at[pl.ds(0, (w1.size + w2.size) * 4 // row_bytes)], send_g)
        wait_bytes(av.at[pl.ds(0, len(peers) * (w1.size + w2.size) * 2 // row_bytes)], send_w)


def tail_kernel(h, n, fw1, fw2, s1, s2, y,
                loss, fw1_out, fw2_out, ow1, ow2, om1, om2, ov1, ov2,
                up, down, sem):
    last = fw1.shape[0] - 1
    outs = [pltpu.make_async_copy(s.at[i], dst, sem)
            for s, dsts in ((s1, (ow1, om1, ov1)), (s2, (ow2, om2, ov2))) for i, dst in enumerate(dsts)]
    outs += [pltpu.make_async_copy(fw1, fw1_out, sem), pltpu.make_async_copy(fw2, fw2_out, sem)]
    for c in outs:
        c.start()
    with jax.named_scope('last'):
        up[...] = fw1[last] * 0.5
        down[...] = fw2[last].astype(F32)
        hidden = mlp_down(mlp_up(n[...], up[...]), h[...].astype(F32), down[...])
        loss[...] = row_mean_sq(hidden.astype(F32) - y[...].astype(F32))
    with jax.named_scope('waitout'):
        moved = (s1.size + s2.size) * 4 + (fw1.size + fw2.size) * 2
        wait_bytes(h.at[pl.ds(0, moved // (h.shape[1] * 2))], sem)


def solution(mesh):
    replicas = mesh.shape['replica']
    grad_spec = P('replica', None, 'data', None)
    shard_spec = P(None, 'data', None)
    row_spec = P(('replica', 'data'), None)
    loss_spec = P(('replica', 'data'))
    full_spec = P()

    def local_step(g1, g2, w1, w2, m1, m2, v1, v2, tokens, targets):
        learn_rate = LR_COEF * tokens.shape[1] ** -0.5
        n_rows, width = tokens.shape
        layers, rows1, hid = w1.shape
        rows2 = w2.shape[1]
        any_ = pl.BlockSpec(memory_space=pl.ANY)
        full1 = (layers, width, hid)
        full2 = (layers, hid, width)
        tiles = n_rows // ROWS
        pieces = 2 * layers - 1 + CUTS
        sh = jax.ShapeDtypeStruct
        dma = pltpu.SemaphoreType.DMA
        vmem = pl.BlockSpec(memory_space=pltpu.VMEM)
        step = pl.pallas_call(
            lambda *refs: step_kernel(learn_rate, replicas, *refs),
            out_shape=[pltpu.VMEM((n_rows, width), BF16), pltpu.VMEM((n_rows, width), BF16), pltpu.VMEM(full1, BF16), pltpu.VMEM(full2, BF16),
                       pltpu.VMEM((3,) + w1.shape, F32), pltpu.VMEM((3,) + w2.shape, F32)],
            in_specs=[any_] * 9,
            out_specs=[vmem] * 6,
            scratch_shapes=[
                pltpu.VMEM(w1.shape, F32), pltpu.VMEM(w2.shape, F32),
                pltpu.VMEM(w1.shape, F32), pltpu.VMEM(w2.shape, F32),
                pltpu.VMEM((n_rows, width), BF16), pltpu.VMEM((n_rows, width), BF16),
                pltpu.VMEM((EARLY_ROWS, hid), F32),
                pltpu.VMEM((width, hid), BF16), pltpu.VMEM((hid, width), F32),
                dma((3,)), dma, dma((2,)),
                dma, dma((pieces,)), dma, dma((pieces,)),
            ],
            compiler_params=pltpu.CompilerParams(
                collective_id=0, has_side_effects=True, vmem_limit_bytes=VMEM_LIMIT),
            name='step',
        )
        mid = step(*(pltpu.with_memory_space_constraint(a, pltpu.HBM)
                     for a in (g1, g2, w1, w2, m1, m2, v1, v2, tokens)))
        mid = [pltpu.with_memory_space_constraint(a, pltpu.VMEM) for a in mid]
        tail = pl.pallas_call(
            tail_kernel,
            out_shape=[sh((1, n_rows), F32), sh(full1, BF16), sh(full2, BF16)]
            + [sh(w1.shape, F32), sh(w2.shape, F32)] * 3,
            in_specs=[vmem] * 7,
            out_specs=[vmem] + [any_] * 8,
            scratch_shapes=[
                pltpu.VMEM((width, hid), BF16), pltpu.VMEM((hid, width), F32),
                dma,
            ],
            compiler_params=pltpu.CompilerParams(vmem_limit_bytes=VMEM_LIMIT),
            name='tail',
        )
        outs = tail(*mid, targets)
        return (outs[0].reshape(n_rows),) + tuple(outs[1:])

    return jax.shard_map(
        local_step,
        mesh=mesh,
        in_specs=(grad_spec, grad_spec, shard_spec, shard_spec, shard_spec, shard_spec, shard_spec, shard_spec, row_spec, row_spec),
        out_specs=(loss_spec, full_spec, full_spec, shard_spec, shard_spec, shard_spec, shard_spec, shard_spec, shard_spec),
        check_vma=False,
    )
```
